32 devices in a mesh: rec: 8 (over z, y), vocab: 4 (over x, core).
Axes of the slice: x: 2, y: 2, z: 4, core: 2. Of those that a mesh axis runs over, the one named last changes fastest.
Arguments:
- features: bfloat16 [32, 192, 1280], P('rec'), may hold values from -1000 to 1000
- head_weight: bfloat16 [1280, 32768], P(None, ('vocab', 'rec')), may hold values from -0.15625 to 0.15625
- labels: int32 [32, 128], P('rec'), may hold values from 0 to 32767
- audio_len: int32 [32], P(('rec', 'vocab')), may hold values from 1 to 192, as said below
- transcript_len: int32 [32], P(('rec', 'vocab')), may hold values from 1 to 128
Outputs:
- label_logprob: float32 [32, 192, 128], P(('rec', 'vocab'))
- path_score: float32 [32], P(('rec', 'vocab'))
The draws below stay inside these ranges and needn't reach their ends.
Inputs may be any that keep to these rules, and one draw needn't show every extreme that they name: `audio_len`: each recording has at least as many frames in use as its transcript has labels.
All inputs are finite; a program needn't handle non-finite values.
Results may differ from the reference program's by a relative error of at most 0.00055.
Values may be sent and summed in bfloat16 or wider, within the bound.
A program may use at most 128 MiB of HBM per device.

```python
import math
import jax
import jax.numpy as jnp
import numpy as np
from jax import lax

D = 1280
VOCAB = 32768
FRAMES = 192
LABELS = 128
REC = 32


def draw_features(key, part):
    key_base = jax.random.fold_in(key, 0)
    values = jnp.clip(jax.random.normal(key_base, (REC, FRAMES, D), jnp.float32), -6.0, 6.0)
    values = values * 3.0
    return values.astype(jnp.bfloat16)


def length_pair(key):
    inner = jax.random.fold_in(key, 7)
    key_text, key_audio = jax.random.split(inner)
    text_len = jax.random.randint(key_text, (REC,), 1, LABELS + 1)
    text_len = text_len.at[1].set(LABELS)
    audio_len = jax.random.randint(key_audio, (REC,), text_len, FRAMES + 1)
    audio_len = jnp.maximum(audio_len, text_len)
    audio_len = audio_len.at[0].set(FRAMES)
    return (audio_len.astype(jnp.int32), text_len.astype(jnp.int32))


def draw_audio_len(key, part):
    return length_pair(key)[0]


def draw_transcript_len(key, part):
    return length_pair(key)[1]


def place_ends(array, rng, least, top_value):
    longest = array.shape.index(max(array.shape))
    spots = []
    for shift in (0, 1):
        where = [jax.random.randint(jax.random.fold_in(rng, axis), (), 0, length) for axis, length in enumerate(array.shape)]
        where[longest] = (where[longest] + shift) % array.shape[longest]
        spots.append(tuple(where))
    return array.at[spots[0]].set(least).at[spots[1]].set(top_value)


def block_levels(stream_key, dims, pieces, least, high):
    gain, own = 1.0, jax.random.fold_in(stream_key, 6)
    for axis_at, shards_of in pieces:
        steps = jnp.exp(jax.random.uniform(jax.random.fold_in(own, axis_at), (shards_of,), jnp.float32, least / len(pieces), high / len(pieces)))
        gain = gain * jnp.repeat(steps, dims[axis_at] // shards_of).reshape([-1 if axis == axis_at else 1 for axis in range(len(dims))])
    return gain


def cumulative_ranks(number_of, skew):
    portions = [(1 << 20) // math.isqrt(grade ** skew) + 1 for grade in range(1, number_of + 1)]
    deviation = 1 + sum(portions) // (1 << 30)
    return np.cumsum(np.array([max(1, weight // deviation) for weight in portions]))


def ranked_ids(rng, shape, amount, lean):
    grid = cumulative_ranks(amount, lean)
    lot = jax.random.randint(jax.random.fold_in(rng, 1), shape, 0, int(grid[amount - 1]))
    grade = jnp.searchsorted(jnp.asarray(grid, jnp.int32), lot, side="right")
    return jax.random.permutation(jax.random.fold_in(rng, 2), amount)[grade].astype(jnp.int32)


def normal_values(key, shape, width, reach, shards=(), dtype=jnp.bfloat16):
    drawn = jax.random.normal(key, shape, jnp.float32) * width
    if len(shards) > 0:
        drawn = block_levels(key, shape, shards, -0.22, 0.18) * drawn
    return jnp.clip(drawn, min=-reach, max=reach).astype(dtype)


def setup_inputs(seed: int = 0) -> dict:
    splits = jax.random.split(jax.random.key(seed), 6)
    return {
        "features": draw_features(jax.random.fold_in(splits[5], 71), 0),
        "head_weight": normal_values(splits[1], (D, VOCAB), D ** -0.5, 0.15625, ((1, 32),)),
        "labels": place_ends(ranked_ids(splits[2], (REC, LABELS), VOCAB, 2), jax.random.fold_in(splits[2], 3), 0, VOCAB - 1).astype(jnp.int32),
        "audio_len": draw_audio_len(jax.random.fold_in(splits[5], 71), 0),
        "transcript_len": draw_transcript_len(jax.random.fold_in(splits[5], 71), 0),
    }


negative_fill = -1e30


def viterbi(log_prob, audio_len, transcript_len):
    rec_count, frames, slots = log_prob.shape
    states = lax.iota(jnp.int32, slots)[None, :]
    target = states == (transcript_len[:, None] - 1)
    initial = jnp.where(states == 0, log_prob[:, 0, :], negative_fill)
    best_end = jnp.where(audio_len == 1, jnp.sum(jnp.where(target, initial, 0.0), 1), 0.0)

    def advance(frame_index, carry):
        current, best_end = carry
        shifted = jnp.concatenate([jnp.full_like(current[:, :1], negative_fill), current[:, :-1]], 1)
        emitted = lax.dynamic_index_in_dim(log_prob, frame_index, 1, keepdims=False)
        current = jnp.maximum(current, shifted) + emitted
        reached = jnp.sum(jnp.where(target, current, 0.0), 1)
        best_end = jnp.where(audio_len - 1 == frame_index, reached, best_end)
        return current, best_end

    current, best_end = lax.fori_loop(1, frames, advance, (initial, best_end))
    return best_end


def reference(features, head_weight, labels, audio_len, transcript_len):
    def per_recording(inputs):
        frame_feats, label_ids = inputs
        logits = jnp.dot(frame_feats, head_weight, preferred_element_type=jnp.float32)
        row_top = jnp.max(logits, 1)
        log_norm = row_top + jnp.log(jnp.sum(jnp.exp(logits - row_top[:, None]), 1))
        picked = jnp.take(logits.astype(jnp.bfloat16), label_ids, axis=1).astype(jnp.float32)
        return picked - log_norm[:, None]

    log_prob = lax.map(per_recording, (features, labels))
    return log_prob, viterbi(log_prob, audio_len, transcript_len)
```

```python
import functools
import jax
import jax.numpy as jnp
from jax import lax
from jax.experimental import pallas as pl
from jax.experimental.pallas import tpu as pltpu
from jax.sharding import PartitionSpec as P

MESH = pl.DeviceIdType.MESH
NEG = -1e30


def flip(v, bit):
    return v + bit * (1 - 2 * ((v // bit) % 2))


def flip_mask(v, mask, bits):
    for bit in bits:
        if mask & bit:
            v = flip(v, bit)
    return v


def gather_kernel(a, b, V, x, w, lab, xo, wo, lo, sw, rw, sl, rl, sf, rf, sg, loc):
    r = lax.axis_index("rec")
    v = lax.axis_index("vocab")
    m, k = r // a, r % a
    own = x.shape[0] // V
    bits = []
    bit = V // 2
    while bit >= 1:
        bits.append(bit)
        bit //= 2
    col_peer = lambda d: (m * a + (k + d) % a, v)
    row_peer = lambda d: (((m + d) % b) * a + k, v)
    barrier = pltpu.get_barrier_semaphore()
    peers = [col_peer(d) for d in range(1, a)] + [row_peer(d) for d in range(1, b)]
    peers += [(r, flip(v, bit)) for bit in bits]
    for peer in peers:
        pl.semaphore_signal(barrier, inc=1, device_id=peer, device_id_type=MESH)
    pl.semaphore_wait(barrier, len(peers))

    def remote(src, dst, ss, rs, to):
        return pltpu.make_async_remote_copy(
            src_ref=src, dst_ref=dst, send_sem=ss, recv_sem=rs, device_id=to, device_id_type=MESH
        )

    sent = []

    def launch(*args):
        c = remote(*args)
        c.start()
        sent.append(c)

    piece = lambda ref, c: ref.at[pl.ds(c * own, own)]
    for d in range(1, b):
        launch(piece(x, v), piece(xo.at[m], v), sf.at[d - 1], rf.at[d - 1, 0], row_peer(d))
    for d in range(1, a):
        launch(w, wo.at[k], sw.at[d - 1], rw.at[d - 1], col_peer(d))
    for d in range(1, b):
        launch(lab, lo.at[m], sl.at[d - 1], rl.at[d - 1], row_peer(d))
    local = [
        pltpu.make_async_copy(x, xo.at[m], loc.at[0]),
        pltpu.make_async_copy(w, wo.at[k], loc.at[1]),
        pltpu.make_async_copy(lab, lo.at[m], loc.at[2]),
    ]
    for c in local:
        c.start()
    order = [0]
    for bit in bits:
        order += [mask | bit for mask in order]
    used = 0
    for mask in order:
        low = (mask & -mask) if mask else V
        c = flip_mask(v, mask, bits)
        for d in range(1, b):
            ms = (m + b - d) % b
            src = piece(xo.at[ms], c)
            remote(src, src, sf.at[d - 1], rf.at[d - 1, mask], row_peer(d)).wait_recv()
            for bit in bits:
                if bit < low:
                    launch(src, src, sg.at[used], rf.at[d - 1, mask | bit], (r, flip(v, bit)))
                    used += 1
    for d in range(1, a):
        ks = (k + a - d) % a
        remote(w, wo.at[ks], sw.at[d - 1], rw.at[d - 1], col_peer(d)).wait_recv()
    for d in range(1, b):
        ms = (m + b - d) % b
        remote(lab, lo.at[ms], sl.at[d - 1], rl.at[d - 1], row_peer(d)).wait_recv()
    for c in sent:
        c.wait_send()
    for c in local:
        c.wait()


def score_kernel(recs, tile, base_ref, x_ref, w_ref, lab_ref, pick_ref, stat_ref, logit):
    a, depth, cols = w_ref.shape
    frames = x_ref.shape[1]
    rows = recs * frames
    xs = x_ref[...].reshape(rows, depth)
    part = None
    acc = [None] * recs
    slots = lab_ref.shape[2]
    for i in range(a):
        for j in range(0, cols, tile):
            l = jnp.dot(xs, w_ref[i, :, j : j + tile], preferred_element_type=jnp.float32)
            at = i * cols + j
            logit[:, at : at + tile] = l
            for n in range(0, tile, 128):
                piece = l[:, n : n + 128]
                part = piece if part is None else jnp.maximum(part, piece)
            low = l.astype(jnp.bfloat16)
            ids = lax.broadcasted_iota(jnp.int32, (tile, slots), 0) + (base_ref[0] + at)
            for q in range(recs):
                hot = (ids == lab_ref[q]).astype(jnp.float32).astype(jnp.bfloat16)
                got = jnp.dot(low[q * frames : (q + 1) * frames], hot, preferred_element_type=jnp.float32)
                acc[q] = got if acc[q] is None else acc[q] + got
    top = jnp.max(part, 1, keepdims=True)
    total = jnp.zeros((rows, 128), jnp.float32)
    for n in range(0, a * cols, 128):
        total = total + jnp.exp(logit[:, n : n + 128] - top)
    total = jnp.sum(total, 1, keepdims=True)
    lane = lax.broadcasted_iota(jnp.int32, (frames, 128), 1)
    for q in range(recs):
        pick_ref[q] = acc[q].astype(jnp.bfloat16)
        part_rows = slice(q * frames, (q + 1) * frames)
        both = jnp.where(lane == 0, top[part_rows], total[part_rows])
        stat_ref[q] = both.T[:8]


def exchange_kernel(a, b, V, pick, stat, po, so, sp, rp, ss, rs, loc):
    r = lax.axis_index("rec")
    v = lax.axis_index("vocab")
    m, k = r // a, r % a
    me = m * V + v
    n = b * V
    peer = lambda d: (((me + d) % n) // V * a + k, (me + d) % V)
    barrier = pltpu.get_barrier_semaphore()
    for d in range(1, n):
        pl.semaphore_signal(barrier, inc=1, device_id=peer(d), device_id_type=MESH)
    pl.semaphore_wait(barrier, n - 1)
    copies = []
    for d in range(1, n):
        to = (me + d) % n
        for src, dst, s, t in ((pick, po, sp, rp), (stat, so, ss, rs)):
            c = pltpu.make_async_remote_copy(
                src_ref=src.at[to], dst_ref=dst.at[me], send_sem=s.at[d - 1], recv_sem=t.at[d - 1],
                device_id=peer(d), device_id_type=MESH,
            )
            c.start()
            copies.append(c)
    local = [
        pltpu.make_async_copy(pick.at[me], po.at[me], loc.at[0]),
        pltpu.make_async_copy(stat.at[me], so.at[me], loc.at[1]),
    ]
    for c in local:
        c.start()
    for d in range(1, n):
        fr = (me + n - d) % n
        for src, dst, s, t in ((pick, po, sp, rp), (stat, so, ss, rs)):
            pltpu.make_async_remote_copy(
                src_ref=src.at[fr], dst_ref=dst.at[fr], send_sem=s.at[d - 1], recv_sem=t.at[d - 1],
                device_id=peer(d), device_id_type=MESH,
            ).wait_recv()
    for c in copies:
        c.wait_send()
    for c in local:
        c.wait()


def align_kernel(alen, tlen, pick, stat, lp_ref, out_ref):
    n, own, frames, slots = pick.shape
    lane = lax.broadcasted_iota(jnp.int32, (1, slots), 1)
    for q in range(own):
        top = stat[0, q, 0:1, :]
        for i in range(1, n):
            top = jnp.maximum(top, stat[i, q, 0:1, :])
        total = jnp.zeros_like(top)
        for i in range(n):
            total = total + stat[i, q, 1:2, :] * jnp.exp(stat[i, q, 0:1, :] - top)
        norm = top + jnp.log(total)
        got = pick[0, q].astype(jnp.float32)
        for i in range(1, n):
            got = got + pick[i, q].astype(jnp.float32)
        lp_ref[q] = got - jnp.broadcast_to(norm, (slots, frames)).T
        last = alen[q] - 1
        first = jnp.where(lane == 0, lp_ref[q, 0:1, :], NEG)

        def advance(t, carry):
            cur, best = carry
            moved = jnp.where(lane == 0, NEG, pltpu.roll(cur, 1, 1))
            cur = jnp.maximum(cur, moved) + lp_ref[q, pl.ds(t, 1), :]
            return cur, jnp.where(last == t, cur, best)

        best = lax.fori_loop(1, frames, advance, (first, first), unroll=4)[1]
        score = jnp.sum(jnp.where(lane == tlen[q] - 1, best, 0.0), 1, keepdims=True)
        out_ref[q] = jnp.broadcast_to(score, (8, 128))


def body(features, head_weight, labels, audio_len, transcript_len):
    rec_dev, frames, width = features.shape
    cols = head_weight.shape[1]
    slots = labels.shape[1]
    G, V = lax.axis_size("rec"), lax.axis_size("vocab")
    best = None
    a = 2
    while a < G:
        cost = (a - 1) * width * cols + (G // a - 1) * features.size
        if G % a == 0 and (best is None or cost < best[0]):
            best = (cost, a)
        a *= 2
    a = best[1]
    b = G // a
    own = rec_dev // V
    vmem = pl.BlockSpec(memory_space=pltpu.VMEM)
    hbm = pl.BlockSpec(memory_space=pl.ANY)
    smem = pl.BlockSpec(memory_space=pltpu.SMEM)
    dma = pltpu.SemaphoreType.DMA
    xg, wg, lg = pl.pallas_call(
        functools.partial(gather_kernel, a, b, V),
        out_shape=(
            jax.ShapeDtypeStruct((b,) + features.shape, features.dtype),
            jax.ShapeDtypeStruct((a,) + head_weight.shape, head_weight.dtype),
            jax.ShapeDtypeStruct((b, rec_dev, 1, slots), jnp.int32),
        ),
        in_specs=[vmem] * 3,
        out_specs=(hbm, hbm, hbm),
        scratch_shapes=[
            dma((a - 1,)), dma((a - 1,)), dma((b - 1,)), dma((b - 1,)),
            dma((b - 1,)), dma((b - 1, V)), dma(((b - 1) * (V - 1),)), dma((3,)),
        ],
        compiler_params=pltpu.CompilerParams(collective_id=0, has_side_effects=True),
        name="gather",
    )(features, head_weight, labels.reshape(rec_dev, 1, slots))

    r, v = lax.axis_index("rec"), lax.axis_index("vocab")
    base = ((v * G + (r // a) * a) * cols).astype(jnp.int32).reshape(1)
    total = b * rec_dev
    recs = 2 if total % 2 == 0 else 1
    tile = min(512, cols)
    pick, stat = pl.pallas_call(
        functools.partial(score_kernel, recs, tile),
        grid=(total // recs,),
        out_shape=(
            jax.ShapeDtypeStruct((total, frames, slots), jnp.bfloat16),
            jax.ShapeDtypeStruct((total, 8, frames), jnp.float32),
        ),
        in_specs=[
            smem,
            pl.BlockSpec((recs, frames, width), lambda i: (i, 0, 0)),
            pl.BlockSpec((a, width, cols), lambda i: (0, 0, 0)),
            pl.BlockSpec((recs, 1, slots), lambda i: (i, 0, 0)),
        ],
        out_specs=(
            pl.BlockSpec((recs, frames, slots), lambda i: (i, 0, 0)),
            pl.BlockSpec((recs, 8, frames), lambda i: (i, 0, 0)),
        ),
        scratch_shapes=[pltpu.VMEM((recs * frames, a * cols), jnp.float32)],
        compiler_params=pltpu.CompilerParams(vmem_limit_bytes=60 * 1024 * 1024),
        name="score",
    )(base, xg.reshape(total, frames, width), wg, lg.reshape(total, 1, slots))

    n = b * V
    pick = pick.reshape(n, own, frames, slots)
    stat = stat.reshape(n, own, 8, frames)
    po, so = pl.pallas_call(
        functools.partial(exchange_kernel, a, b, V),
        out_shape=(
            jax.ShapeDtypeStruct(pick.shape, pick.dtype),
            jax.ShapeDtypeStruct(stat.shape, stat.dtype),
        ),
        in_specs=[vmem] * 2,
        out_specs=(vmem, vmem),
        scratch_shapes=[dma((n - 1,))] * 4 + [dma((2,))],
        compiler_params=pltpu.CompilerParams(collective_id=1, has_side_effects=True),
        name="exchange",
    )(pick, stat)

    log_prob, score = pl.pallas_call(
        align_kernel,
        out_shape=(
            jax.ShapeDtypeStruct((own, frames, slots), jnp.float32),
            jax.ShapeDtypeStruct((own, 8, 128), jnp.float32),
        ),
        in_specs=[smem, smem, vmem, vmem],
        out_specs=(vmem, vmem),
        name="align",
    )(audio_len, transcript_len, po, so)
    return log_prob, score[:, 0, 0]


def solution(mesh):
    return jax.shard_map(
        body,
        mesh=mesh,
        in_specs=(
            P("rec", None, None),
            P(None, ("vocab", "rec")),
            P("rec", None),
            P(("rec", "vocab")),
            P(("rec", "vocab")),
        ),
        out_specs=(P(("rec", "vocab"), None, None), P(("rec", "vocab"))),
        check_vma=False,
    )
```

```python
import functools
import jax
import jax.numpy as jnp
from jax import lax
from jax.experimental import pallas as pl
from jax.experimental.pallas import tpu as pltpu
from jax.sharding import PartitionSpec as P

MESH = pl.DeviceIdType.MESH
NEG = -1e30
run = 6


def flip(v, bit):
    return v + bit * (1 - 2 * ((v // bit) % 2))


def flip_mask(v, mask, bits):
    for bit in bits:
        if mask & bit:
            v = flip(v, bit)
    return v


def gather_kernel(a, b, V, x, w, lab, xo, wo, lo, sw, rw, sl, rl, sf, rf, sg, loc):
    r = lax.axis_index("rec")
    v = lax.axis_index("vocab")
    m, k = r // a, r % a
    own = x.shape[0] // V
    bits = []
    bit = V // 2
    while bit >= 1:
        bits.append(bit)
        bit //= 2
    col_peer = lambda d: (m * a + (k + d) % a, v)
    row_peer = lambda d: (((m + d) % b) * a + k, v)
    barrier = pltpu.get_barrier_semaphore()
    peers = [col_peer(d) for d in range(1, a)] + [row_peer(d) for d in range(1, b)]
    peers += [(r, flip(v, bit)) for bit in bits]
    for peer in peers:
        pl.semaphore_signal(barrier, inc=1, device_id=peer, device_id_type=MESH)
    pl.semaphore_wait(barrier, len(peers))

    def remote(src, dst, ss, rs, to):
        return pltpu.make_async_remote_copy(
            src_ref=src, dst_ref=dst, send_sem=ss, recv_sem=rs, device_id=to, device_id_type=MESH
        )

    sent = []

    def launch(*args):
        c = remote(*args)
        c.start()
        sent.append(c)

    piece = lambda ref, c: ref.at[pl.ds(c * own, own)]
    for d in range(1, b):
        launch(piece(x, v), piece(xo.at[m], v), sf.at[d - 1], rf.at[d - 1, 0], row_peer(d))
    for d in range(1, a):
        launch(w, wo.at[k], sw.at[d - 1], rw.at[d - 1], col_peer(d))
    for d in range(1, b):
        launch(lab, lo.at[m], sl.at[d - 1], rl.at[d - 1], row_peer(d))
    local = [
        pltpu.make_async_copy(x, xo.at[m], loc.at[0]),
        pltpu.make_async_copy(w, wo.at[k], loc.at[1]),
        pltpu.make_async_copy(lab, lo.at[m], loc.at[2]),
    ]
    for c in local:
        c.start()
    order = [0]
    for bit in bits:
        order += [mask | bit for mask in order]
    used = 0
    for mask in order:
        low = (mask & -mask) if mask else V
        c = flip_mask(v, mask, bits)
        for d in range(1, b):
            ms = (m + b - d) % b
            src = piece(xo.at[ms], c)
            remote(src, src, sf.at[d - 1], rf.at[d - 1, mask], row_peer(d)).wait_recv()
            for bit in bits:
                if bit < low:
                    launch(src, src, sg.at[used], rf.at[d - 1, mask | bit], (r, flip(v, bit)))
                    used += 1
    for d in range(1, a):
        ks = (k + a - d) % a
        remote(w, wo.at[ks], sw.at[d - 1], rw.at[d - 1], col_peer(d)).wait_recv()
    for d in range(1, b):
        ms = (m + b - d) % b
        remote(lab, lo.at[ms], sl.at[d - 1], rl.at[d - 1], row_peer(d)).wait_recv()
    for c in sent:
        c.wait_send()
    for c in local:
        c.wait()


def score_kernel(recs, tile, base_ref, x_ref, w_ref, lab_ref, pick_ref, stat_ref, logit):
    a, depth, cols = w_ref.shape
    frames = x_ref.shape[1]
    rows = recs * frames
    xs = x_ref[...].reshape(rows, depth)
    part = None
    acc = [None] * recs
    slots = lab_ref.shape[2]
    for i in range(a):
        for j in range(0, cols, tile):
            l = jnp.dot(xs, w_ref[i, :, j : j + tile], preferred_element_type=jnp.float32)
            at = i * cols + j
            logit[:, at : at + tile] = l
            for n in range(0, tile, 128):
                piece = l[:, n : n + 128]
                part = piece if part is None else jnp.maximum(part, piece)
            low = l.astype(jnp.bfloat16)
            ids = lax.broadcasted_iota(jnp.int32, (tile, slots), 0) + (base_ref[0] + at)
            for q in range(recs):
                hot = (ids == lab_ref[q]).astype(jnp.float32).astype(jnp.bfloat16)
                got = jnp.dot(low[q * frames : (q + 1) * frames], hot, preferred_element_type=jnp.float32)
                acc[q] = got if acc[q] is None else acc[q] + got
    top = jnp.max(part, 1, keepdims=True)
    total = jnp.zeros((rows, 128), jnp.float32)
    for n in range(0, a * cols, 128):
        total = total + jnp.exp(logit[:, n : n + 128] - top)
    total = jnp.sum(total, 1, keepdims=True)
    lane = lax.broadcasted_iota(jnp.int32, (frames, 128), 1)
    for q in range(recs):
        pick_ref[q] = acc[q].astype(jnp.bfloat16)
        part_rows = slice(q * frames, (q + 1) * frames)
        both = jnp.where(lane == 0, top[part_rows], total[part_rows])
        stat_ref[q] = both.T[:8]


def exchange_kernel(a, b, V, pick, stat, po, so, pin, sin, pout, sout, sp1, rp1, ss1, rs1, sp, rp, ss, rs):
    r = lax.axis_index("rec")
    v = lax.axis_index("vocab")
    m, k = r // a, r % a
    half = V // 2
    side = v % 2
    me = m * half + v // 2
    n = b * half
    sibling = (r, flip(v, 1))
    peer = lambda d: (((me + d) % n) // half * a + k, ((me + d) % n) % half * 2 + side)
    barrier = pltpu.get_barrier_semaphore()
    for to in [sibling] + [peer(d) for d in range(1, n)]:
        pl.semaphore_signal(barrier, inc=1, device_id=to, device_id_type=MESH)
    pl.semaphore_wait(barrier, n)

    def remote(src, dst, s, t, to):
        return pltpu.make_async_remote_copy(
            src_ref=src, dst_ref=dst, send_sem=s, recv_sem=t, device_id=to, device_id_type=MESH
        )

    copies = []
    for e in range(n):
        copies.append(remote(pick.at[e, 1 - side], pin.at[e], sp1.at[e], rp1.at[e], sibling))
        copies.append(remote(stat.at[e, 1 - side], sin.at[e], ss1.at[e], rs1.at[e], sibling))
    for c in copies:
        c.start()
    row = lax.broadcasted_iota(jnp.int32, sin.shape[1:], 1)
    for e in range(n):
        copies[2 * e].wait_recv()
        copies[2 * e + 1].wait_recv()
        pout[e] = pick[e, side] + pin[e]
        mine, other = stat[e, side], sin[e]
        top = jnp.maximum(mine[:, 0:1], other[:, 0:1])
        total = mine * jnp.exp(mine[:, 0:1] - top) + other * jnp.exp(other[:, 0:1] - top)
        sout[e] = jnp.where(row == 0, top, total)
    for d in range(1, n):
        to = (me + d) % n
        for src, dst, s, t in ((pout, po, sp, rp), (sout, so, ss, rs)):
            c = remote(src.at[to], dst.at[me], s.at[d - 1], t.at[d - 1], peer(d))
            c.start()
            copies.append(c)
    po[me] = pout[me]
    so[me] = sout[me]
    for d in range(1, n):
        fr = (me + n - d) % n
        for src, dst, s, t in ((pout, po, sp, rp), (sout, so, ss, rs)):
            remote(src.at[fr], dst.at[fr], s.at[d - 1], t.at[d - 1], peer(d)).wait_recv()
    for c in copies:
        c.wait_send()


def align_kernel(alen, tlen, pick, stat, lp_ref, out_ref):
    n, own, frames, slots = pick.shape
    lane = lax.broadcasted_iota(jnp.int32, (1, slots), 1)
    for q in range(own):
        top = stat[0, q, 0:1, :]
        for i in range(1, n):
            top = jnp.maximum(top, stat[i, q, 0:1, :])
        total = jnp.zeros_like(top)
        for i in range(n):
            total = total + stat[i, q, 1:2, :] * jnp.exp(stat[i, q, 0:1, :] - top)
        norm = top + jnp.log(total)
        got = pick[0, q].astype(jnp.float32)
        for i in range(1, n):
            got = got + pick[i, q].astype(jnp.float32)
        lp_ref[q] = got - jnp.broadcast_to(norm, (slots, frames)).T
        last = alen[q] - 1
        first = jnp.where(lane == 0, lp_ref[q, 0:1, :], NEG)

        def block(t, steps, cur, best):
            emit = [lp_ref[q, pl.ds(t + i, 1), :] for i in range(steps)]
            rolled = [[e if c == 0 else pltpu.roll(e, c, 1) for c in range(steps - i)] for i, e in enumerate(emit)]
            moved = [cur] + [jnp.where(lane < c, NEG, pltpu.roll(cur, c, 1)) for c in range(1, steps + 1)]
            for i in range(steps):
                moved = [jnp.maximum(moved[c], moved[c + 1]) + rolled[i][c] for c in range(steps - i)]
                best = jnp.where(last == t + i, moved[0], best)
            return moved[0], best

        whole = (frames - 1) // run
        cur, best = lax.fori_loop(0, whole, lambda i, c: block(1 + i * run, run, *c), (first, first))
        if (frames - 1) % run:
            best = block(1 + whole * run, (frames - 1) % run, cur, best)[1]
        score = jnp.sum(jnp.where(lane == tlen[q] - 1, best, 0.0), 1, keepdims=True)
        out_ref[q] = jnp.broadcast_to(score, (8, 128))


def body(features, head_weight, labels, audio_len, transcript_len):
    rec_dev, frames, width = features.shape
    cols = head_weight.shape[1]
    slots = labels.shape[1]
    G, V = lax.axis_size("rec"), lax.axis_size("vocab")
    best = None
    a = 2
    while a < G:
        cost = (a - 1) * width * cols + (G // a - 1) * features.size
        if G % a == 0 and (best is None or cost < best[0]):
            best = (cost, a)
        a *= 2
    a = best[1]
    b = G // a
    own = rec_dev // V
    vmem = pl.BlockSpec(memory_space=pltpu.VMEM)
    hbm = pl.BlockSpec(memory_space=pl.ANY)
    smem = pl.BlockSpec(memory_space=pltpu.SMEM)
    dma = pltpu.SemaphoreType.DMA
    xg, wg, lg = pl.pallas_call(
        functools.partial(gather_kernel, a, b, V),
        out_shape=(
            jax.ShapeDtypeStruct((b,) + features.shape, features.dtype),
            jax.ShapeDtypeStruct((a,) + head_weight.shape, head_weight.dtype),
            jax.ShapeDtypeStruct((b, rec_dev, 1, slots), jnp.int32),
        ),
        in_specs=[vmem] * 3,
        out_specs=(hbm, hbm, hbm),
        scratch_shapes=[
            dma((a - 1,)), dma((a - 1,)), dma((b - 1,)), dma((b - 1,)),
            dma((b - 1,)), dma((b - 1, V)), dma(((b - 1) * (V - 1),)), dma((3,)),
        ],
        compiler_params=pltpu.CompilerParams(collective_id=0, has_side_effects=True),
        name="gather",
    )(features, head_weight, labels.reshape(rec_dev, 1, slots))

    r, v = lax.axis_index("rec"), lax.axis_index("vocab")
    base = ((v * G + (r // a) * a) * cols).astype(jnp.int32).reshape(1)
    total = b * rec_dev
    recs = 2 if total % 2 == 0 else 1
    tile = min(512, cols)
    pick, stat = pl.pallas_call(
        functools.partial(score_kernel, recs, tile),
        grid=(total // recs,),
        out_shape=(
            jax.ShapeDtypeStruct((total, frames, slots), jnp.bfloat16),
            jax.ShapeDtypeStruct((total, 8, frames), jnp.float32),
        ),
        in_specs=[
            smem,
            pl.BlockSpec((recs, frames, width), lambda i: (i, 0, 0)),
            pl.BlockSpec((a, width, cols), lambda i: (0, 0, 0)),
            pl.BlockSpec((recs, 1, slots), lambda i: (i, 0, 0)),
        ],
        out_specs=(
            pl.BlockSpec((recs, frames, slots), lambda i: (i, 0, 0)),
            pl.BlockSpec((recs, 8, frames), lambda i: (i, 0, 0)),
        ),
        scratch_shapes=[pltpu.VMEM((recs * frames, a * cols), jnp.float32)],
        compiler_params=pltpu.CompilerParams(vmem_limit_bytes=60 * 1024 * 1024),
        name="score",
    )(base, xg.reshape(total, frames, width), wg, lg.reshape(total, 1, slots))

    n = b * (V // 2)
    pick = pick.reshape(n, 2, own, frames, slots)
    stat = stat.reshape(n, 2, own, 8, frames)
    picked = (n, own, frames, slots)
    stats = (n, own, 8, frames)
    po, so = pl.pallas_call(
        functools.partial(exchange_kernel, a, b, V),
        out_shape=(
            jax.ShapeDtypeStruct(picked, pick.dtype),
            jax.ShapeDtypeStruct(stats, stat.dtype),
        ),
        in_specs=[vmem] * 2,
        out_specs=(vmem, vmem),
        scratch_shapes=[pltpu.VMEM(picked, pick.dtype), pltpu.VMEM(stats, stat.dtype)] * 2
        + [dma((n,))] * 4
        + [dma((n - 1,))] * 4,
        compiler_params=pltpu.CompilerParams(collective_id=1, has_side_effects=True),
        name="exchange",
    )(pick, stat)

    log_prob, score = pl.pallas_call(
        align_kernel,
        out_shape=(
            jax.ShapeDtypeStruct((own, frames, slots), jnp.float32),
            jax.ShapeDtypeStruct((own, 8, 128), jnp.float32),
        ),
        in_specs=[smem, smem, vmem, vmem],
        out_specs=(vmem, vmem),
        name="align",
    )(audio_len, transcript_len, po, so)
    return log_prob, score[:, 0, 0]


def solution(mesh):
    return jax.shard_map(
        body,
        mesh=mesh,
        in_specs=(
            P("rec", None, None),
            P(None, ("vocab", "rec")),
            P("rec", None),
            P(("rec", "vocab")),
            P(("rec", "vocab")),
        ),
        out_specs=(P(("rec", "vocab"), None, None), P(("rec", "vocab"))),
        check_vma=False,
    )
```
